32 devices in a mesh: layer: 4 (over x, core), tok: 8 (over z, y).
Axes of the slice: x: 2, y: 2, z: 4, core: 2. Of those that a mesh axis runs over, the one named last changes fastest.
Arguments:
- kv_cache: bfloat16 [4, 2, 2, 1, 1024, 1024], P('layer', None, None, None, 'tok'), may hold values from -6 to 6
- keep_mask: int32 [4, 1, 1024], P('layer', None, 'tok'), may hold values 0 or 1
- lengths: int32 [1], replicated, may hold values from 256 to 1024
Outputs:
- decode_cache: bfloat16 [1, 8, 8, 2, 1024, 128], P(None, 'layer', None, None, 'tok')
The draws below stay inside these ranges and needn't reach their ends.
Inputs may be any that keep to these rules, and one draw needn't show every extreme that they name: `keep_mask`: 1 keeps the token of both layers of the pair unmerged. `lengths`: positions at or past a sequence's length are padding.
All inputs are finite; a program needn't handle non-finite values. No bound on the sum of `keep_mask` on one device may be relied on, other than what follows from the above.
Results may differ from the reference program's by a relative error of at most 0.001.
Values may be sent and summed in bfloat16 or wider, within the bound.
No kernel may reach another device: no remote copies, remote signals or barrier semaphores. Data moves between devices by JAX's collectives and lax.ppermute only.
A program may use at most 64 MiB of HBM per device.

```python
import jax
import jax.numpy as jnp
from jax import lax

KVH = 8
HD = 128
PAGE = 16
SEQS = 1
PAIRS = 4
LEN = 1024
N_TOK = 8


def touch_ends(array, rng, smallest, top_value):
    longest = array.shape.index(max(array.shape))
    spots = []
    for shift in (0, 1):
        where = [jax.random.randint(jax.random.fold_in(rng, axis), (), 0, length) for axis, length in enumerate(array.shape)]
        where[longest] = (where[longest] + shift) % array.shape[longest]
        spots.append(tuple(where))
    return array.at[spots[0]].set(smallest).at[spots[1]].set(top_value)


def level_of(rng, extent, cuts, smallest, largest):
    def one(dim, shards_of):
        heights = jax.random.uniform(jax.random.fold_in(jax.random.fold_in(rng, 6), dim), (shards_of,), jnp.float32, smallest / len(cuts), largest / len(cuts))
        return jnp.repeat(jnp.exp(heights), extent[dim] // shards_of).reshape((-1,) + (1,) * (len(extent) - dim - 1))

    level = one(*cuts[0])
    for cut in cuts[1:]:
        level = level * one(*cut)
    return level


def centred(stream_key, extent, scale, limit, shards=(), held_as=jnp.bfloat16):
    loudness = level_of(stream_key, extent, shards, -0.22, 0.18) if shards else 1.0
    entries = jax.random.normal(stream_key, extent, jnp.float32) * scale * loudness
    return jnp.minimum(jnp.maximum(entries, -limit), limit).astype(held_as)


def setup_inputs(seed: int = 0) -> dict:
    splits = jax.random.split(jax.random.key(seed), 4)
    kv_cache = centred(splits[0], (PAIRS, 2, 2, SEQS, LEN, KVH * HD), 1.0, 6.0, ((0, 4), (4, 8)))
    keep_mask = touch_ends((jax.random.randint(splits[1], (PAIRS, SEQS, LEN), 0, 8) < 1).astype(jnp.int32), jax.random.fold_in(splits[1], 1), 0, 1)
    lengths = jax.random.randint(splits[2], (SEQS,), LEN // 4, LEN + 1).astype(jnp.int32)
    return {"kv_cache": kv_cache, "keep_mask": keep_mask, "lengths": lengths}


epsilon = 1e-06

def merge_pair(lower_layer, upper_layer, retained, inside):
    lower_scale = jnp.sqrt(lax.optimization_barrier(jnp.mean(lower_layer * lower_layer, axis=-1, keepdims=True)) + epsilon)
    upper_scale = jnp.sqrt(lax.optimization_barrier(jnp.mean(upper_layer * upper_layer, axis=-1, keepdims=True)) + epsilon)
    summed = lower_layer / lower_scale + upper_layer / upper_scale
    direction = summed / jnp.sqrt(lax.optimization_barrier(jnp.mean(summed * summed, axis=-1, keepdims=True)) + epsilon)
    lower_out = jnp.where(retained, lower_layer, lower_scale * direction)
    upper_out = jnp.where(retained, upper_layer, upper_scale * direction)
    lower_out = jnp.where(inside, lower_out, jnp.zeros_like(lower_out))
    upper_out = jnp.where(inside, upper_out, jnp.zeros_like(upper_out))
    return jnp.stack([lower_out, upper_out], axis=0).astype(jnp.bfloat16)

def reference(kv_cache, keep_mask, lengths):
    position = jnp.arange(LEN, dtype=jnp.int32)
    inside = (position[None, :] < lengths[:, None])[None, :, :, None, None]

    def one_pair(operands):
        pair_cache, pair_keep = operands
        values = pair_cache.astype(jnp.float32).reshape(2, 2, SEQS, LEN, KVH, HD)
        retained = (pair_keep > 0)[None, :, :, None, None]
        return merge_pair(values[0], values[1], retained, inside)
    merged = lax.map(one_pair, (kv_cache, keep_mask))
    rounds = LEN // (N_TOK * PAGE)
    merged = merged.reshape(PAIRS, 2, 2, SEQS, rounds, N_TOK, PAGE, KVH, HD)
    ordered = merged.transpose(3, 7, 0, 1, 2, 5, 4, 6, 8)
    return ordered.reshape(SEQS, KVH, 2 * PAIRS, 2, LEN, HD)
```

```python
import functools

import jax
import jax.numpy as jnp
from jax import lax
from jax.experimental import pallas as pl
from jax.experimental.pallas import tpu as pltpu
from jax.sharding import PartitionSpec as P

KVH = 8
HD = 128
PAGE = 16


epsilon = 1e-06


def column(row, rows):
    parts = [
        jnp.broadcast_to(row[:, k : k + HD], (HD, HD)).T for k in range(0, rows, HD)
    ]
    return parts[0] if len(parts) == 1 else jnp.concatenate(parts, axis=0)


def merge_kernel(first_ref, length_ref, keep_ref, values_ref, out_ref, *, head_group):
    rows = values_ref.shape[2]
    pages = rows // PAGE
    keep = column((keep_ref[...] > 0).astype(jnp.float32), rows)
    position = first_ref[0] + lax.broadcasted_iota(jnp.int32, (rows, HD), 0)
    inside = position < length_ref[0]
    retained = jnp.logical_and(keep > 0.0, inside)
    live = inside.astype(jnp.float32)
    for head in range(KVH):
        lanes = slice(head * HD, (head + 1) * HD)
        lower = values_ref[0, 0, :, lanes].astype(jnp.float32)
        upper = values_ref[1, 0, :, lanes].astype(jnp.float32)
        lower_square = jnp.mean(lower * lower, axis=-1, keepdims=True) + epsilon
        upper_square = jnp.mean(upper * upper, axis=-1, keepdims=True) + epsilon
        lower_inverse = lax.rsqrt(lower_square)
        upper_inverse = lax.rsqrt(upper_square)
        summed = lower * lower_inverse + upper * upper_inverse
        summed_inverse = lax.rsqrt(jnp.mean(summed * summed, axis=-1, keepdims=True) + epsilon)
        direction = summed * (summed_inverse * live)
        lower_out = jnp.where(retained, lower, (lower_square * lower_inverse) * direction)
        upper_out = jnp.where(retained, upper, (upper_square * upper_inverse) * direction)
        group, member = head // head_group, head % head_group
        out_ref[group, :, member, 0, 0] = lower_out.astype(jnp.bfloat16).reshape(pages, PAGE, HD)
        out_ref[group, :, member, 1, 0] = upper_out.astype(jnp.bfloat16).reshape(pages, PAGE, HD)


def merged_pages(values, keep, lengths, first, groups):
    rows = values.shape[2]
    head_group = KVH // groups
    pages = rows // PAGE
    return pl.pallas_call(
        functools.partial(merge_kernel, head_group=head_group),
        grid=(2,),
        in_specs=[
            pl.BlockSpec(memory_space=pltpu.SMEM),
            pl.BlockSpec(memory_space=pltpu.SMEM),
            pl.BlockSpec((1, rows), lambda c: (0, 0)),
            pl.BlockSpec((2, 1, rows, KVH * HD), lambda c: (0, c, 0, 0)),
        ],
        out_specs=pl.BlockSpec(
            (groups, pages, head_group, 2, 1, PAGE, HD), lambda c: (0, 0, 0, 0, c, 0, 0)
        ),
        out_shape=jax.ShapeDtypeStruct(
            (groups, pages, head_group, 2, 2, PAGE, HD), jnp.bfloat16
        ),
    )(first, lengths, keep, values)


def shards(kv_cache, keep_mask, lengths):
    groups = lax.axis_size("layer")
    tok_count = lax.axis_size("tok")
    seq_count = kv_cache.shape[3]
    rows_dev = kv_cache.shape[4]
    head_group = KVH // groups
    rounds = rows_dev // (PAGE * tok_count)
    first = (lax.axis_index("tok") * rows_dev).astype(jnp.int32).reshape(1)
    pieces = []
    for s in range(seq_count):
        pages = merged_pages(
            kv_cache[0, :, :, s], keep_mask[0, s : s + 1], lengths[s : s + 1], first, groups
        )
        pages = pages.reshape(groups, rounds, tok_count, -1)
        pieces.append(pages.transpose(0, 2, 1, 3))
    outgoing = jnp.stack(pieces, axis=2)
    shape = (groups, tok_count, seq_count, rounds, head_group, 2, 2, PAGE, HD)
    flat = outgoing.reshape((groups * tok_count, -1) + shape[-2:])
    arrived = lax.all_to_all(
        flat, ("layer", "tok"), split_axis=0, concat_axis=0, tiled=True
    ).reshape(shape)
    result = arrived.transpose(2, 4, 0, 5, 6, 1, 3, 7, 8)
    return result.reshape(seq_count, head_group, 2 * groups, 2, rows_dev, HD)


def solution(mesh):
    in_specs = (P("layer", None, None, None, "tok", None), P("layer", None, "tok"), P())
    out_specs = P(None, "layer", None, None, "tok", None)
    return jax.shard_map(shards, mesh=mesh, in_specs=in_specs, out_specs=out_specs, check_vma=False)
```

```python
import functools

import jax
import jax.numpy as jnp
from jax import lax
from jax.experimental import pallas as pl
from jax.experimental.pallas import tpu as pltpu
from jax.sharding import PartitionSpec as P

KVH = 8
HD = 128
PAGE = 16


epsilon = 1e-06

VMEM_GRANT = 16 * 2**20


def merge(lower, upper, retained, live):
    lower_square = jnp.mean(lower * lower, axis=-1, keepdims=True) + epsilon
    upper_square = jnp.mean(upper * upper, axis=-1, keepdims=True) + epsilon
    lower_inverse = lax.rsqrt(lower_square)
    upper_inverse = lax.rsqrt(upper_square)
    summed = lower * lower_inverse + upper * upper_inverse
    summed_inverse = lax.rsqrt(jnp.mean(summed * summed, axis=-1, keepdims=True) + epsilon)
    direction = summed * (summed_inverse * live)
    lower_out = jnp.where(retained, lower, (lower_square * lower_inverse) * direction)
    upper_out = jnp.where(retained, upper, (upper_square * upper_inverse) * direction)
    return lower_out.astype(jnp.bfloat16), upper_out.astype(jnp.bfloat16)


def merge_kernel(place_ref, length_ref, keep_ref, values_ref, *rest, plan, groups, tok_count, rounds):
    outs, (loaded, columns, sems) = rest[: len(plan)], rest[len(plan) :]
    layer, tok = place_ref[0], place_ref[1]
    rows_dev = values_ref.shape[2]
    head_group = KVH // groups
    width = head_group * HD
    offsets = sorted({k for entry in plan for _, k in entry})
    run = rounds * PAGE

    def copies(j):
        lanes = pl.ds(pl.multiple_of((layer ^ j) * width, width), width)
        for n, k in enumerate(offsets):
            for r in range(rounds):
                source = pl.ds(pl.multiple_of((r * tok_count + (tok ^ k)) * PAGE, PAGE), PAGE)
                target = pl.ds(n * run + r * PAGE, PAGE)
                yield pltpu.make_async_copy(
                    values_ref.at[:, :, source, lanes], loaded.at[j, :, :, target, :], sems.at[j, n, r]
                )

    for j in range(groups):
        for copy in copies(j):
            copy.start()
    for block in range(0, rows_dev, HD):
        keep = (keep_ref[:, block : block + HD] > 0).astype(jnp.float32)
        columns[block : block + HD, :] = jnp.broadcast_to(keep, (HD, HD)).T
    row = lax.broadcasted_iota(jnp.int32, (PAGE, HD), 0)
    retained, live = [], []
    for k in offsets:
        for r in range(rounds):
            start = pl.multiple_of((r * tok_count + (tok ^ k)) * PAGE, PAGE)
            inside = (row + (tok * rows_dev + start)) < length_ref[0]
            live.append(inside.astype(jnp.float32))
            kept = columns[pl.ds(start, PAGE), :]
            retained.append(kept * live[-1])
    retained = jnp.concatenate(retained, axis=0) > 0.0
    live = jnp.concatenate(live, axis=0)
    where = {}
    for o, entry in enumerate(plan):
        for n, piece in enumerate(entry):
            where[piece] = (o, n)
    for j in range(groups):
        for copy in copies(j):
            copy.wait()
        for c in range(2):
            for member in range(head_group):
                lanes = slice(member * HD, (member + 1) * HD)
                both = merge(
                    loaded[j, 0, c, :, lanes].astype(jnp.float32),
                    loaded[j, 1, c, :, lanes].astype(jnp.float32),
                    retained,
                    live,
                )
                for side in range(2):
                    for n, k in enumerate(offsets):
                        o, slot = where[(j, k)]
                        outs[o][slot, :, member, side, c] = both[side][n * run : (n + 1) * run].reshape(rounds, PAGE, HD)


def merged(values, keep, lengths, place, plan, groups, tok_count):
    rows_dev = values.shape[2]
    rounds = rows_dev // (PAGE * tok_count)
    head_group = KVH // groups
    count = len({k for entry in plan for _, k in entry})
    return pl.pallas_call(
        functools.partial(merge_kernel, plan=plan, groups=groups, tok_count=tok_count, rounds=rounds),
        in_specs=[
            pl.BlockSpec(memory_space=pltpu.SMEM),
            pl.BlockSpec(memory_space=pltpu.SMEM),
            pl.BlockSpec(memory_space=pltpu.VMEM),
            pl.BlockSpec(memory_space=pltpu.HBM),
        ],
        out_specs=[pl.BlockSpec(memory_space=pltpu.VMEM) for _ in plan],
        out_shape=[
            jax.ShapeDtypeStruct((len(entry), rounds, head_group, 2, 2, PAGE, HD), jnp.bfloat16)
            for entry in plan
        ],
        scratch_shapes=[
            pltpu.VMEM((groups, 2, 2, count * rounds * PAGE, head_group * HD), jnp.bfloat16),
            pltpu.VMEM((rows_dev, HD), jnp.float32),
            pltpu.SemaphoreType.DMA((groups, count, rounds)),
        ],
        compiler_params=pltpu.CompilerParams(vmem_limit_bytes=VMEM_GRANT),
    )(place, lengths, keep, values)


def place_kernel(place_ref, *rest, plan, rounds):
    pieces, out_ref, sems = rest[: len(plan)], rest[len(plan)], rest[len(plan) + 1]
    layer, tok = place_ref[0], place_ref[1]

    def copies():
        n = 0
        for piece_ref, entry in zip(pieces, plan):
            for slot, (j, k) in enumerate(entry):
                for r in range(rounds):
                    pair = pl.ds((layer ^ j) * 2, 2)
                    rows = pl.ds(pl.multiple_of(((tok ^ k) * rounds + r) * PAGE, PAGE), PAGE)
                    yield pltpu.make_async_copy(
                        piece_ref.at[slot, r], out_ref.at[:, pair, :, rows, :], sems.at[n]
                    )
                    n += 1

    for copy in copies():
        copy.start()
    for copy in copies():
        copy.wait()


def placed(pieces, place, plan, groups, rows_dev):
    rounds, head_group = pieces[0].shape[1], pieces[0].shape[2]
    count = sum(len(entry) for entry in plan) * rounds
    return pl.pallas_call(
        functools.partial(place_kernel, plan=plan, rounds=rounds),
        in_specs=[pl.BlockSpec(memory_space=pltpu.SMEM)]
        + [pl.BlockSpec(memory_space=pltpu.VMEM) for _ in pieces],
        out_specs=pl.BlockSpec(memory_space=pltpu.HBM),
        out_shape=jax.ShapeDtypeStruct((head_group, 2 * groups, 2, rows_dev, HD), jnp.bfloat16),
        scratch_shapes=[pltpu.SemaphoreType.DMA((count,))],
        compiler_params=pltpu.CompilerParams(vmem_limit_bytes=VMEM_GRANT),
    )(place, *pieces)


def one_sequence(values, keep, lengths, groups, tok_count):
    rows_dev = values.shape[2]
    place = jnp.stack([lax.axis_index("layer"), lax.axis_index("tok")]).astype(jnp.int32)
    half, quarter = tok_count // 2, tok_count // 4
    early = list(range(half, half + quarter))
    late = list(range(half + quarter, tok_count))
    near = list(range(half))
    layers = range(groups)

    def over_layer(array, j):
        return lax.ppermute(array, "layer", [(i, i ^ j) for i in range(groups)])

    def over_tok(array, k):
        return lax.ppermute(array, "tok", [(i, i ^ k) for i in range(tok_count)])

    first = merged(values, keep, lengths, place, [[(j, k) for j in layers] for k in early], groups, tok_count)
    early_in = [over_tok(array, k) for array, k in zip(first, early)]
    second = merged(
        values, keep, lengths, place,
        [[(j, k) for k in late] for j in layers] + [[(j, k) for k in near] for j in layers],
        groups, tok_count,
    )
    late_mine = [over_layer(second[j], j) if j else second[j] for j in layers]
    near_mine = [over_layer(second[groups + j], j) if j else second[groups + j] for j in layers]
    late_in = [
        over_tok(jnp.concatenate([array[n : n + 1] for array in late_mine]), k) for n, k in enumerate(late)
    ]
    near_in = [
        over_tok(jnp.concatenate([array[n : n + 1] for array in near_mine]), k)
        for n, k in enumerate(near)
        if k
    ]
    early_mine = [
        over_layer(jnp.concatenate([array[j : j + 1] for array in early_in]), j) for j in layers if j
    ]
    pieces, plan = [], []
    for array, j in zip(early_mine, [j for j in layers if j]):
        pieces.append(array)
        plan.append([(j, k) for k in early])
    for array, k in zip(early_in, early):
        pieces.append(array[:1])
        plan.append([(0, k)])
    for array, k in zip(late_in, late):
        pieces.append(array)
        plan.append([(j, k) for j in layers])
    for array, k in zip(near_in, near[1:]):
        pieces.append(array)
        plan.append([(j, k) for j in layers])
    for array, j in zip(near_mine, layers):
        pieces.append(array[:1])
        plan.append([(j, 0)])
    return placed(pieces, place, plan, groups, rows_dev)


def shards(kv_cache, keep_mask, lengths):
    groups = lax.axis_size("layer")
    tok_count = lax.axis_size("tok")
    seq_count = kv_cache.shape[3]
    return jnp.stack(
        [
            one_sequence(kv_cache[0, :, :, s], keep_mask[0, s : s + 1], lengths[s : s + 1], groups, tok_count)
            for s in range(seq_count)
        ]
    )


def solution(mesh):
    in_specs = (P("layer", None, None, None, "tok", None), P("layer", None, "tok"), P())
    out_specs = P(None, "layer", None, None, "tok", None)
    return jax.shard_map(shards, mesh=mesh, in_specs=in_specs, out_specs=out_specs, check_vma=False)
```

```python
import functools

import jax
import jax.numpy as jnp
from jax import lax
from jax.experimental import pallas as pl
from jax.experimental.pallas import tpu as pltpu
from jax.sharding import PartitionSpec as P


KVH = 8
HD = 128
PAGE = 16


epsilon = 1e-06

VMEM_GRANT = 16 * 2**20


def merge(lower, upper, retained, live):
    lower_square = jnp.mean(lower * lower, axis=-1, keepdims=True) + epsilon
    upper_square = jnp.mean(upper * upper, axis=-1, keepdims=True) + epsilon
    lower_inverse = lax.rsqrt(lower_square)
    upper_inverse = lax.rsqrt(upper_square)
    summed = lower * lower_inverse + upper * upper_inverse
    summed_inverse = lax.rsqrt(jnp.mean(summed * summed, axis=-1, keepdims=True) + epsilon)
    direction = summed * (summed_inverse * live)
    lower_out = jnp.where(retained, lower, (lower_square * lower_inverse) * direction)
    upper_out = jnp.where(retained, upper, (upper_square * upper_inverse) * direction)
    return lower_out.astype(jnp.bfloat16), upper_out.astype(jnp.bfloat16)


def merge_kernel(length_ref, keep_ref, values_ref, *rest, plan, groups, tok_count, rounds):
    outs, (loaded, mask, columns, sems, mask_sem) = rest[: len(plan)], rest[len(plan) :]
    layer, tok = lax.axis_index("layer"), lax.axis_index("tok")
    rows_dev = values_ref.shape[2]
    head_group = KVH // groups
    width = head_group * HD
    offsets = sorted({k for entry in plan for _, k in entry})
    run = rounds * PAGE

    def copies(j):
        lanes = pl.ds(pl.multiple_of((layer ^ j) * width, width), width)
        for n, k in enumerate(offsets):
            for r in range(rounds):
                source = pl.ds(pl.multiple_of((r * tok_count + (tok ^ k)) * PAGE, PAGE), PAGE)
                target = pl.ds(n * run + r * PAGE, PAGE)
                yield pltpu.make_async_copy(
                    values_ref.at[:, :, source, lanes], loaded.at[j, :, :, target, :], sems.at[j, n, r]
                )

    mask_copy = pltpu.make_async_copy(keep_ref, mask, mask_sem)
    mask_copy.start()
    for j in range(groups):
        for copy in copies(j):
            copy.start()
    mask_copy.wait()
    for block in range(0, rows_dev, HD):
        keep = (mask[:, block : block + HD] > 0).astype(jnp.float32)
        columns[block : block + HD, :] = jnp.broadcast_to(keep, (HD, HD)).T
    row = lax.broadcasted_iota(jnp.int32, (PAGE, HD), 0)
    retained, live = [], []
    for k in offsets:
        for r in range(rounds):
            start = pl.multiple_of((r * tok_count + (tok ^ k)) * PAGE, PAGE)
            inside = (row + (tok * rows_dev + start)) < length_ref[0]
            live.append(inside.astype(jnp.float32))
            kept = columns[pl.ds(start, PAGE), :]
            retained.append(kept * live[-1])
    retained = jnp.concatenate(retained, axis=0) > 0.0
    live = jnp.concatenate(live, axis=0)
    where = {}
    for o, entry in enumerate(plan):
        for n, piece in enumerate(entry):
            where[piece] = (o, n)
    for j in range(groups):
        for copy in copies(j):
            copy.wait()
        for c in range(2):
            for member in range(head_group):
                lanes = slice(member * HD, (member + 1) * HD)
                both = merge(
                    loaded[j, 0, c, :, lanes].astype(jnp.float32),
                    loaded[j, 1, c, :, lanes].astype(jnp.float32),
                    retained,
                    live,
                )
                for side in range(2):
                    for n, k in enumerate(offsets):
                        o, slot = where[(j, k)]
                        outs[o][slot, :, member, side, c] = both[side][n * run : (n + 1) * run].reshape(rounds, PAGE, HD)


def merged(values, keep, lengths, plan, groups, tok_count):
    rows_dev = values.shape[2]
    rounds = rows_dev // (PAGE * tok_count)
    head_group = KVH // groups
    count = len({k for entry in plan for _, k in entry})
    return pl.pallas_call(
        functools.partial(merge_kernel, plan=plan, groups=groups, tok_count=tok_count, rounds=rounds),
        in_specs=[
            pl.BlockSpec(memory_space=pltpu.SMEM),
            pl.BlockSpec(memory_space=pltpu.HBM),
            pl.BlockSpec(memory_space=pltpu.HBM),
        ],
        out_specs=[pl.BlockSpec(memory_space=pltpu.VMEM) for _ in plan],
        out_shape=[
            jax.ShapeDtypeStruct((len(entry), rounds, head_group, 2, 2, PAGE, HD), jnp.bfloat16)
            for entry in plan
        ],
        scratch_shapes=[
            pltpu.VMEM((groups, 2, 2, count * rounds * PAGE, head_group * HD), jnp.bfloat16),
            pltpu.VMEM((1, rows_dev), jnp.int32),
            pltpu.VMEM((rows_dev, HD), jnp.float32),
            pltpu.SemaphoreType.DMA((groups, count, rounds)),
            pltpu.SemaphoreType.DMA(()),
        ],
        compiler_params=pltpu.CompilerParams(vmem_limit_bytes=VMEM_GRANT),
    )(lengths, *[pltpu.with_memory_space_constraint(array, pltpu.HBM) for array in (keep, values)])


def place_kernel(*rest, plan, rounds, chained):
    pieces = rest[: len(plan)]
    out_ref, sems = rest[len(plan) + chained :]
    layer, tok = lax.axis_index("layer"), lax.axis_index("tok")

    def copies():
        n = 0
        for piece_ref, entry in zip(pieces, plan):
            for slot, (j, k) in enumerate(entry):
                for r in range(rounds):
                    pair = pl.ds((layer ^ j) * 2, 2)
                    rows = pl.ds(pl.multiple_of(((tok ^ k) * rounds + r) * PAGE, PAGE), PAGE)
                    yield pltpu.make_async_copy(
                        piece_ref.at[slot, r], out_ref.at[:, pair, :, rows, :], sems.at[n]
                    )
                    n += 1

    for copy in copies():
        copy.start()
    for copy in copies():
        copy.wait()


def placed(pieces, groups, rows_dev, before=None):
    arrays, plan = [array for array, _ in pieces], [entry for _, entry in pieces]
    rounds, head_group = arrays[0].shape[1], arrays[0].shape[2]
    count = sum(len(entry) for entry in plan) * rounds
    chained = before is not None
    return pl.pallas_call(
        functools.partial(place_kernel, plan=plan, rounds=rounds, chained=int(chained)),
        in_specs=[pl.BlockSpec(memory_space=pltpu.VMEM) for _ in arrays]
        + [pl.BlockSpec(memory_space=pltpu.HBM)] * chained,
        out_specs=pl.BlockSpec(memory_space=pltpu.HBM),
        out_shape=jax.ShapeDtypeStruct((head_group, 2 * groups, 2, rows_dev, HD), jnp.bfloat16),
        scratch_shapes=[pltpu.SemaphoreType.DMA((count,))],
        input_output_aliases={len(arrays): 0} if chained else {},
        compiler_params=pltpu.CompilerParams(vmem_limit_bytes=VMEM_GRANT),
    )(*arrays, *([before] if chained else []))


def offsets_of(groups, tok_count):
    half, quarter = tok_count // 2, tok_count // 4
    early = list(range(half, half + quarter))
    late = list(range(half + quarter, tok_count))
    near = list(range(half))
    return [j for j in range(groups - 1, 0, -1)], early, late, near


def one_sequence(values, keep, lengths, groups, tok_count):
    rows_dev = values.shape[2]
    _, early, late, near = offsets_of(groups, tok_count)
    layers = range(groups)

    def over_layer(array, j):
        return lax.ppermute(array, "layer", [(i, i ^ j) for i in range(groups)])

    def over_tok(array, k):
        return lax.ppermute(array, "tok", [(i, i ^ k) for i in range(tok_count)])

    def joined(arrays, n):
        return jnp.concatenate([array[n : n + 1] for array in arrays])

    def merge_into(plan):
        return merged(values, keep, lengths, plan, groups, tok_count)

    first = merge_into([[(j, early[0]) for j in layers]])
    second = merge_into(
        [[(j, k) for k in late] for j in layers] + [[(j, k) for j in layers] for k in early[1:]],
    )
    third = merge_into([[(j, k) for k in near] for j in layers])
    early_in = [over_tok(array, k) for array, k in zip([*first, *second[groups:]], early)]
    late_mine = [second[0]] + [over_layer(second[j], j) for j in layers if j]
    near_mine = [third[0]] + [over_layer(third[j], j) for j in layers if j]
    late_in = [over_tok(joined(late_mine, n), k) for n, k in enumerate(late)]
    near_in = [over_tok(joined(near_mine, n), k) for n, k in enumerate(near) if k]
    early_mine = [over_layer(joined(early_in, j), j) for j in layers if j]
    out = placed(
        [(array[:1], [(0, k)]) for array, k in zip(early_in, early)]
        + [(array[:1], [(j, 0)]) for array, j in zip(near_mine, layers)]
        + [(array, [(j, k) for j in layers]) for array, k in zip(near_in, near[1:])],
        groups, rows_dev,
    )
    return placed(
        [(array, [(j, k) for k in early]) for array, j in zip(early_mine, layers[1:])]
        + [(array, [(j, k) for j in layers]) for array, k in zip(late_in, late)],
        groups, rows_dev, before=out,
    )


def shards(kv_cache, keep_mask, lengths):
    groups = lax.axis_size("layer")
    tok_count = lax.axis_size("tok")
    seq_count = kv_cache.shape[3]
    return jnp.stack(
        [
            one_sequence(kv_cache[0, :, :, s], keep_mask[0, s : s + 1], lengths[s : s + 1], groups, tok_count)
            for s in range(seq_count)
        ]
    )


def solution(mesh):
    in_specs = (P("layer", None, None, None, "tok", None), P("layer", None, "tok"), P())
    out_specs = P(None, "layer", None, None, "tok", None)
    return jax.shard_map(shards, mesh=mesh, in_specs=in_specs, out_specs=out_specs, check_vma=False)
```

```python
import functools

import jax
import jax.numpy as jnp
from jax import lax
from jax.experimental import pallas as pl
from jax.experimental.pallas import tpu as pltpu
from jax.sharding import PartitionSpec as P


KVH = 8
HD = 128
PAGE = 16


epsilon = 1e-06

VMEM_GRANT = 16 * 2**20


def merge(lower, upper, retained, live):
    lower_square = jnp.mean(lower * lower, axis=-1, keepdims=True) + epsilon
    upper_square = jnp.mean(upper * upper, axis=-1, keepdims=True) + epsilon
    lower_inverse = lax.rsqrt(lower_square)
    upper_inverse = lax.rsqrt(upper_square)
    summed = lower * lower_inverse + upper * upper_inverse
    summed_inverse = lax.rsqrt(jnp.mean(summed * summed, axis=-1, keepdims=True) + epsilon)
    direction = summed * (summed_inverse if live is None else summed_inverse * live)
    lower_out = jnp.where(retained, lower, (lower_square * lower_inverse) * direction)
    upper_out = jnp.where(retained, upper, (upper_square * upper_inverse) * direction)
    return lower_out.astype(jnp.bfloat16), upper_out.astype(jnp.bfloat16)


def merge_kernel(*refs, plan, groups, tok_count, rounds, limited):
    keep_ref, values_ref, *rest = refs[limited:]
    outs, (loaded, mask, columns, sems, mask_sem) = rest[: len(plan)], rest[len(plan) :]
    layer, tok = lax.axis_index("layer"), lax.axis_index("tok")
    rows_dev = values_ref.shape[2]
    head_group = KVH // groups
    width = head_group * HD
    offsets = sorted({k for entry in plan for _, k in entry})
    run = rounds * PAGE

    def copies(j):
        lanes = pl.ds(pl.multiple_of((layer ^ j) * width, width), width)
        for n, k in enumerate(offsets):
            for r in range(rounds):
                source = pl.ds(pl.multiple_of((r * tok_count + (tok ^ k)) * PAGE, PAGE), PAGE)
                target = pl.ds(n * run + r * PAGE, PAGE)
                yield pltpu.make_async_copy(
                    values_ref.at[:, :, source, lanes], loaded.at[j, :, :, target, :], sems.at[j, n, r]
                )

    mask_copy = pltpu.make_async_copy(keep_ref, mask, mask_sem)
    mask_copy.start()
    for j in range(groups):
        for copy in copies(j):
            copy.start()
    mask_copy.wait()
    for block in range(0, rows_dev, HD):
        keep = (mask[:, block : block + HD] > 0).astype(jnp.float32)
        columns[block : block + HD, :] = jnp.broadcast_to(keep, (HD, HD)).T
    row = lax.broadcasted_iota(jnp.int32, (PAGE, HD), 0)
    retained, live = [], []
    for k in offsets:
        for r in range(rounds):
            start = pl.multiple_of((r * tok_count + (tok ^ k)) * PAGE, PAGE)
            retained.append(columns[pl.ds(start, PAGE), :])
            if limited:
                inside = (row + (tok * rows_dev + start)) < refs[0][0]
                live.append(inside.astype(jnp.float32))
                retained[-1] *= live[-1]
    retained = jnp.concatenate(retained, axis=0) > 0.0
    live = jnp.concatenate(live, axis=0) if limited else None
    where = {}
    for o, entry in enumerate(plan):
        for n, piece in enumerate(entry):
            where[piece] = (o, n)
    for j in range(groups):
        for copy in copies(j):
            copy.wait()
        for c in range(2):
            for member in range(head_group):
                lanes = slice(member * HD, (member + 1) * HD)
                both = merge(
                    loaded[j, 0, c, :, lanes].astype(jnp.float32),
                    loaded[j, 1, c, :, lanes].astype(jnp.float32),
                    retained,
                    live,
                )
                for side in range(2):
                    for n, k in enumerate(offsets):
                        o, slot = where[(j, k)]
                        outs[o][slot, :, member, side, c] = both[side][n * run : (n + 1) * run].reshape(rounds, PAGE, HD)


def merged(values, keep, lengths, plan, groups, tok_count):
    rows_dev = values.shape[2]
    rounds = rows_dev // (PAGE * tok_count)
    head_group = KVH // groups
    count = len({k for entry in plan for _, k in entry})
    return pl.pallas_call(
        functools.partial(merge_kernel, plan=plan, groups=groups, tok_count=tok_count, rounds=rounds, limited=len(lengths)),
        in_specs=[
            *[pl.BlockSpec(memory_space=pltpu.SMEM) for _ in lengths],
            pl.BlockSpec(memory_space=pltpu.HBM),
            pl.BlockSpec(memory_space=pltpu.HBM),
        ],
        out_specs=[pl.BlockSpec(memory_space=pltpu.VMEM) for _ in plan],
        out_shape=[
            jax.ShapeDtypeStruct((len(entry), rounds, head_group, 2, 2, PAGE, HD), jnp.bfloat16)
            for entry in plan
        ],
        scratch_shapes=[
            pltpu.VMEM((groups, 2, 2, count * rounds * PAGE, head_group * HD), jnp.bfloat16),
            pltpu.VMEM((1, rows_dev), jnp.int32),
            pltpu.VMEM((rows_dev, HD), jnp.float32),
            pltpu.SemaphoreType.DMA((groups, count, rounds)),
            pltpu.SemaphoreType.DMA(()),
        ],
        compiler_params=pltpu.CompilerParams(vmem_limit_bytes=VMEM_GRANT),
    )(*lengths, *[pltpu.with_memory_space_constraint(array, pltpu.HBM) for array in (keep, values)])


def place_kernel(*rest, plan, rounds, chained):
    pieces = rest[: len(plan)]
    out_ref, sems = rest[len(plan) + chained :]
    layer, tok = lax.axis_index("layer"), lax.axis_index("tok")

    def copies():
        n = 0
        for piece_ref, entry in zip(pieces, plan):
            for slot, (j, k) in enumerate(entry):
                for r in range(rounds):
                    pair = pl.ds((layer ^ j) * 2, 2)
                    rows = pl.ds(pl.multiple_of(((tok ^ k) * rounds + r) * PAGE, PAGE), PAGE)
                    yield pltpu.make_async_copy(
                        piece_ref.at[slot, r], out_ref.at[:, pair, :, rows, :], sems.at[n]
                    )
                    n += 1

    for copy in copies():
        copy.start()
    for copy in copies():
        copy.wait()


def placed(pieces, groups, rows_dev, before=None):
    arrays, plan = [array for array, _ in pieces], [entry for _, entry in pieces]
    rounds, head_group = arrays[0].shape[1], arrays[0].shape[2]
    count = sum(len(entry) for entry in plan) * rounds
    chained = before is not None
    return pl.pallas_call(
        functools.partial(place_kernel, plan=plan, rounds=rounds, chained=int(chained)),
        in_specs=[pl.BlockSpec(memory_space=pltpu.VMEM) for _ in arrays]
        + [pl.BlockSpec(memory_space=pltpu.HBM)] * chained,
        out_specs=pl.BlockSpec(memory_space=pltpu.HBM),
        out_shape=jax.ShapeDtypeStruct((head_group, 2 * groups, 2, rows_dev, HD), jnp.bfloat16),
        scratch_shapes=[pltpu.SemaphoreType.DMA((count,))],
        input_output_aliases={len(arrays): 0} if chained else {},
        compiler_params=pltpu.CompilerParams(vmem_limit_bytes=VMEM_GRANT),
    )(*arrays, *([before] if chained else []))


def offsets_of(groups, tok_count):
    half, quarter = tok_count // 2, tok_count // 4
    small = list(range(quarter))
    middle = list(range(quarter, half))
    early = list(range(half, half + quarter))
    late = list(range(half + quarter, tok_count))
    return list(range(groups - 1, 0, -1)), small, middle, early, late


def one_sequence(values, keep, lengths, groups, tok_count):
    rows_dev = values.shape[2]
    _, small, middle, early, late = offsets_of(groups, tok_count)
    layers = range(groups)

    def over_layer(array, j):
        return lax.ppermute(array, "layer", [(i, i ^ j) for i in range(groups)])

    def over_tok(array, k):
        return lax.ppermute(array, "tok", [(i, i ^ k) for i in range(tok_count)])

    def joined(arrays, n):
        return jnp.concatenate([array[n : n + 1] for array in arrays])

    def merge_into(plan, limits):
        return merged(values, keep, limits, plan, groups, tok_count)

    def without_padding(array, k):
        rounds = array.shape[1]
        tok = lax.axis_index("tok")
        first = (tok ^ k) * rows_dev + tok * PAGE
        shape = (1, rounds, 1, 1, 1, PAGE, HD)
        position = first + lax.broadcasted_iota(jnp.int32, shape, 5)
        position += lax.broadcasted_iota(jnp.int32, shape, 1) * (PAGE * tok_count)
        return jnp.where(position < lengths[0], array, jnp.zeros_like(array))

    first = merge_into([[(j, k) for j in layers] for k in early], [])
    lengths, first = lax.optimization_barrier((lengths, first))
    second = merge_into([[(j, k) for k in late] for j in layers], [lengths])
    third = merge_into(
        [[(j, k) for j in layers] for k in middle] + [[(j, k) for k in small] for j in layers], [lengths]
    )
    early_in = [without_padding(over_tok(array, k), k) for array, k in zip(first, early)]
    late_mine = [second[0]] + [over_layer(second[j], j) for j in layers if j]
    middle_in = [over_tok(array, k) for array, k in zip(third, middle)]
    small_mine = third[len(middle) :]
    small_mine = [small_mine[0]] + [over_layer(small_mine[j], j) for j in layers if j]
    late_in = [over_tok(joined(late_mine, n), k) for n, k in enumerate(late)]
    small_in = [over_tok(joined(small_mine, n), k) for n, k in enumerate(small) if k]
    relayed = middle + early
    relayed_mine = [over_layer(joined(middle_in + early_in, j), j) for j in layers if j]
    out = placed(
        [(array[:1], [(0, k)]) for array, k in zip(middle_in + early_in, relayed)]
        + [(array[:1], [(j, 0)]) for array, j in zip(small_mine, layers)]
        + [(array, [(j, k) for j in layers]) for array, k in zip(small_in, small[1:])]
        + [(array, [(j, k) for k in relayed]) for array, j in zip(relayed_mine, layers[1:])],
        groups, rows_dev,
    )
    return placed(
        [(array, [(j, k) for j in layers]) for array, k in zip(late_in, late)],
        groups, rows_dev, before=out,
    )


def shards(kv_cache, keep_mask, lengths):
    groups = lax.axis_size("layer")
    tok_count = lax.axis_size("tok")
    seq_count = kv_cache.shape[3]
    return jnp.stack(
        [
            one_sequence(kv_cache[0, :, :, s], keep_mask[0, s : s + 1], lengths[s : s + 1], groups, tok_count)
            for s in range(seq_count)
        ]
    )


def solution(mesh):
    in_specs = (P("layer", None, None, None, "tok", None), P("layer", None, "tok"), P())
    out_specs = P(None, "layer", None, None, "tok", None)
    return jax.shard_map(shards, mesh=mesh, in_specs=in_specs, out_specs=out_specs, check_vma=False)
```

```python
import functools

import jax
import jax.numpy as jnp
from jax import lax
from jax.experimental import pallas as pl
from jax.experimental.pallas import tpu as pltpu
from jax.sharding import PartitionSpec as P


KVH = 8
HD = 128
PAGE = 16


epsilon = 1e-06

VMEM_GRANT = 16 * 2**20


def merge(lower, upper, retained, live):
    lower_square = jnp.mean(lower * lower, axis=-1, keepdims=True) + epsilon
    upper_square = jnp.mean(upper * upper, axis=-1, keepdims=True) + epsilon
    lower_inverse = lax.rsqrt(lower_square)
    upper_inverse = lax.rsqrt(upper_square)
    summed = lower * lower_inverse + upper * upper_inverse
    summed_inverse = lax.rsqrt(jnp.mean(summed * summed, axis=-1, keepdims=True) + epsilon)
    direction = summed * (summed_inverse if live is None else summed_inverse * live)
    lower_out = jnp.where(retained, lower, (lower_square * lower_inverse) * direction)
    upper_out = jnp.where(retained, upper, (upper_square * upper_inverse) * direction)
    return lower_out.astype(jnp.bfloat16), upper_out.astype(jnp.bfloat16)


def merge_kernel(*refs, plan, groups, tok_count, rounds, limited):
    keep_ref, values_ref, *rest = refs[limited:]
    outs, (loaded, mask, columns, sems, mask_sem) = rest[: len(plan)], rest[len(plan) :]
    layer, tok = lax.axis_index("layer"), lax.axis_index("tok")
    rows_dev = values_ref.shape[2]
    head_group = KVH // groups
    width = head_group * HD
    offsets = sorted({k for entry in plan for _, k in entry})
    run = rounds * PAGE

    def copies(j):
        lanes = pl.ds(pl.multiple_of((layer ^ j) * width, width), width)
        for n, k in enumerate(offsets):
            for r in range(rounds):
                source = pl.ds(pl.multiple_of((r * tok_count + (tok ^ k)) * PAGE, PAGE), PAGE)
                target = pl.ds(n * run + r * PAGE, PAGE)
                yield pltpu.make_async_copy(
                    values_ref.at[:, :, source, lanes], loaded.at[j, :, :, target, :], sems.at[j, n, r]
                )

    mask_copy = pltpu.make_async_copy(keep_ref, mask, mask_sem)
    mask_copy.start()
    for j in range(groups):
        for copy in copies(j):
            copy.start()
    mask_copy.wait()
    for block in range(0, rows_dev, HD):
        keep = (mask[:, block : block + HD] > 0).astype(jnp.float32)
        columns[block : block + HD, :] = jnp.broadcast_to(keep, (HD, HD)).T
    row = lax.broadcasted_iota(jnp.int32, (PAGE, HD), 0)
    retained, live = [], []
    for k in offsets:
        for r in range(rounds):
            start = pl.multiple_of((r * tok_count + (tok ^ k)) * PAGE, PAGE)
            retained.append(columns[pl.ds(start, PAGE), :])
            if limited:
                inside = (row + (tok * rows_dev + start)) < refs[0][0]
                live.append(inside.astype(jnp.float32))
                retained[-1] *= live[-1]
    retained = jnp.concatenate(retained, axis=0) > 0.0
    live = jnp.concatenate(live, axis=0) if limited else None
    where = {}
    for o, entry in enumerate(plan):
        for n, piece in enumerate(entry):
            where[piece] = (o, n)
    for j in range(groups):
        for copy in copies(j):
            copy.wait()
        for c in range(2):
            for member in range(head_group):
                lanes = slice(member * HD, (member + 1) * HD)
                both = merge(
                    loaded[j, 0, c, :, lanes].astype(jnp.float32),
                    loaded[j, 1, c, :, lanes].astype(jnp.float32),
                    retained,
                    live,
                )
                for side in range(2):
                    for n, k in enumerate(offsets):
                        o, slot = where[(j, k)]
                        outs[o][slot, :, member, side, c] = both[side][n * run : (n + 1) * run].reshape(rounds, PAGE, HD)


def merged(values, keep, lengths, plan, groups, tok_count):
    rows_dev = values.shape[2]
    rounds = rows_dev // (PAGE * tok_count)
    head_group = KVH // groups
    count = len({k for entry in plan for _, k in entry})
    return pl.pallas_call(
        functools.partial(merge_kernel, plan=plan, groups=groups, tok_count=tok_count, rounds=rounds, limited=len(lengths)),
        in_specs=[
            *[pl.BlockSpec(memory_space=pltpu.SMEM) for _ in lengths],
            pl.BlockSpec(memory_space=pltpu.HBM),
            pl.BlockSpec(memory_space=pltpu.HBM),
        ],
        out_specs=[pl.BlockSpec(memory_space=pltpu.VMEM) for _ in plan],
        out_shape=[
            jax.ShapeDtypeStruct((len(entry), rounds, head_group, 2, 2, PAGE, HD), jnp.bfloat16)
            for entry in plan
        ],
        scratch_shapes=[
            pltpu.VMEM((groups, 2, 2, count * rounds * PAGE, head_group * HD), jnp.bfloat16),
            pltpu.VMEM((1, rows_dev), jnp.int32),
            pltpu.VMEM((rows_dev, HD), jnp.float32),
            pltpu.SemaphoreType.DMA((groups, count, rounds)),
            pltpu.SemaphoreType.DMA(()),
        ],
        compiler_params=pltpu.CompilerParams(vmem_limit_bytes=VMEM_GRANT),
    )(*lengths, *[pltpu.with_memory_space_constraint(array, pltpu.HBM) for array in (keep, values)])


def place_kernel(*rest, plan, rounds, chained):
    pieces = rest[: len(plan)]
    out_ref, sems = rest[len(plan) + chained :]
    layer, tok = lax.axis_index("layer"), lax.axis_index("tok")

    def copies():
        n = 0
        for piece_ref, entry in zip(pieces, plan):
            for slot, offset in enumerate(entry):
                if offset is None:
                    continue
                j, k = offset
                for r in range(rounds):
                    pair = pl.ds((layer ^ j) * 2, 2)
                    rows = pl.ds(pl.multiple_of(((tok ^ k) * rounds + r) * PAGE, PAGE), PAGE)
                    yield pltpu.make_async_copy(
                        piece_ref.at[slot, r], out_ref.at[:, pair, :, rows, :], sems.at[n]
                    )
                    n += 1

    for copy in copies():
        copy.start()
    for copy in copies():
        copy.wait()


def placed(pieces, groups, rows_dev, before=None):
    arrays, plan = [array for array, _ in pieces], [entry for _, entry in pieces]
    rounds, head_group = arrays[0].shape[1], arrays[0].shape[2]
    count = sum(len(entry) for entry in plan) * rounds
    chained = before is not None
    return pl.pallas_call(
        functools.partial(place_kernel, plan=plan, rounds=rounds, chained=int(chained)),
        in_specs=[pl.BlockSpec(memory_space=pltpu.VMEM) for _ in arrays]
        + [pl.BlockSpec(memory_space=pltpu.HBM)] * chained,
        out_specs=pl.BlockSpec(memory_space=pltpu.HBM),
        out_shape=jax.ShapeDtypeStruct((head_group, 2 * groups, 2, rows_dev, HD), jnp.bfloat16),
        scratch_shapes=[pltpu.SemaphoreType.DMA((count,))],
        input_output_aliases={len(arrays): 0} if chained else {},
        compiler_params=pltpu.CompilerParams(vmem_limit_bytes=VMEM_GRANT),
    )(*arrays, *([before] if chained else []))


def offsets_of(groups, tok_count):
    half, quarter = tok_count // 2, tok_count // 4
    near = list(range(half))
    early = list(range(half, half + quarter))
    late = list(range(half + quarter, tok_count))
    return list(range(groups - 1, 0, -1)), near, early, late


def one_sequence(values, keep, lengths, groups, tok_count):
    rows_dev = values.shape[2]
    _, near, early, late = offsets_of(groups, tok_count)
    layers = range(groups)

    def over_layer(array, j):
        return lax.ppermute(array, "layer", [(i, i ^ j) for i in range(groups)])

    def over_tok(array, k):
        return lax.ppermute(array, "tok", [(i, i ^ k) for i in range(tok_count)])

    def joined(arrays, n):
        return jnp.concatenate([array[n : n + 1] for array in arrays])

    def merge_into(plan, limits):
        return merged(values, keep, limits, plan, groups, tok_count)

    def without_padding(array, k, source):
        rounds = array.shape[1]
        first = source * rows_dev + (source ^ k) * PAGE
        shape = (1, rounds, 1, 1, 1, PAGE, HD)
        position = first + lax.broadcasted_iota(jnp.int32, shape, 5)
        position += lax.broadcasted_iota(jnp.int32, shape, 1) * (PAGE * tok_count)
        return jnp.where(position < lengths[0], array, jnp.zeros_like(array))

    tok = lax.axis_index("tok")
    first = merge_into([[(j, k) for j in layers] for k in early] + [[(j, k) for k in late] for j in layers], [])
    lengths, first = lax.optimization_barrier((lengths, first))
    second = merge_into([[(j, k) for k in near] for j in layers], [lengths])
    early_in = [over_tok(array, k) for array, k in zip(first, early)]
    early_in = [without_padding(array, k, tok ^ k) for array, k in zip(early_in, early)]
    late_mine = first[len(early) :]
    late_mine = [late_mine[0]] + [over_layer(late_mine[j], j) for j in layers if j]
    near_mine = [second[0]] + [over_layer(second[j], j) for j in layers if j]
    late_in = [over_tok(without_padding(joined(late_mine, n), k, tok), k) for n, k in enumerate(late)]
    early_mine = [over_layer(joined(early_in, j), j) for j in layers if j]
    near_in = [over_tok(joined(near_mine, n), k) for n, k in enumerate(near) if k]
    out = placed(
        [(array[:1], [(0, k)]) for array, k in zip(early_in, early)]
        + [(array[:1], [(j, 0)]) for array, j in zip(near_mine, layers)]
        + [(array, [(j, k) for k in early]) for array, j in zip(early_mine, layers[1:])],
        groups, rows_dev,
    )
    return placed(
        [(array, [(j, k) for j in layers]) for array, k in zip(late_in + near_in, late + near[1:])],
        groups, rows_dev, before=out,
    )


def shards(kv_cache, keep_mask, lengths):
    groups = lax.axis_size("layer")
    tok_count = lax.axis_size("tok")
    seq_count = kv_cache.shape[3]
    return jnp.stack(
        [
            one_sequence(kv_cache[0, :, :, s], keep_mask[0, s : s + 1], lengths[s : s + 1], groups, tok_count)
            for s in range(seq_count)
        ]
    )


def solution(mesh):
    in_specs = (P("layer", None, None, None, "tok", None), P("layer", None, "tok"), P())
    out_specs = P(None, "layer", None, None, "tok", None)
    return jax.shard_map(shards, mesh=mesh, in_specs=in_specs, out_specs=out_specs, check_vma=False)
```

```python
import functools

import jax
import jax.numpy as jnp
from jax import lax
from jax.experimental import pallas as pl
from jax.experimental.pallas import tpu as pltpu
from jax.sharding import PartitionSpec as P


KVH = 8
HD = 128
PAGE = 16


epsilon = 1e-06

VMEM_GRANT = 16 * 2**20


def merge(lower, upper, retained):
    lower_square = jnp.mean(lower * lower, axis=-1, keepdims=True) + epsilon
    upper_square = jnp.mean(upper * upper, axis=-1, keepdims=True) + epsilon
    lower_inverse = lax.rsqrt(lower_square)
    upper_inverse = lax.rsqrt(upper_square)
    summed = lower * lower_inverse + upper * upper_inverse
    summed_inverse = lax.rsqrt(jnp.mean(summed * summed, axis=-1, keepdims=True) + epsilon)
    direction = summed * summed_inverse
    lower_out = jnp.where(retained, lower, (lower_square * lower_inverse) * direction)
    upper_out = jnp.where(retained, upper, (upper_square * upper_inverse) * direction)
    return lower_out.astype(jnp.bfloat16), upper_out.astype(jnp.bfloat16)


def merge_kernel(keep_ref, values_ref, *rest, plan, always, lower, upper, groups, tok_count, rounds):
    loaded, mask, columns, sems, mask_sem = rest[-5:]
    outs = rest[-5 - len(plan) : -5]
    layer, tok = lax.axis_index("layer"), lax.axis_index("tok")
    rows_dev = values_ref.shape[2]
    head_group = KVH // groups
    width = head_group * HD
    where = {}
    for o, entry in enumerate(plan):
        for n, piece in enumerate(entry):
            where[piece] = (o, n)
    slots = {k: n for n, k in enumerate(always + lower + upper)}

    def copies(k):
        n = slots[k]
        for r in range(rounds):
            source = pl.ds(pl.multiple_of((r * tok_count + (tok ^ k)) * PAGE, PAGE), PAGE)
            yield pltpu.make_async_copy(values_ref.at[:, :, source, :], loaded.at[n, r], sems.at[n, r])

    mask_copy = pltpu.make_async_copy(keep_ref, mask, mask_sem)

    def load(offsets):
        for k in offsets:
            for copy in copies(k):
                copy.start()

    def turn_mask():
        mask_copy.wait()
        for block in range(0, rows_dev, HD):
            keep = (mask[:, block : block + HD] > 0).astype(jnp.float32)
            columns[block : block + HD, :] = jnp.broadcast_to(keep, (HD, HD)).T

    def work(offsets):
        for k in offsets:
            for copy in copies(k):
                copy.wait()
            n = slots[k]
            for r in range(rounds):
                start = pl.multiple_of((r * tok_count + (tok ^ k)) * PAGE, PAGE)
                retained = columns[pl.ds(start, PAGE), :] > 0.0
                for j in range(groups):
                    o, slot = where[(j, k)]
                    for c in range(2):
                        for member in range(head_group):
                            lane = pl.multiple_of((layer ^ j) * width + member * HD, HD)
                            both = merge(
                                loaded[n, r, 0, c, :, pl.ds(lane, HD)].astype(jnp.float32),
                                loaded[n, r, 1, c, :, pl.ds(lane, HD)].astype(jnp.float32),
                                retained,
                            )
                            for side in range(2):
                                outs[o][slot, r, member, side, c] = both[side]

    if always:
        mask_copy.start()
        load(always)
        if lower:
            pl.when(tok < tok_count // 2)(lambda: load(lower))
        turn_mask()
        work(always)
        if lower:
            pl.when(tok < tok_count // 2)(lambda: work(lower))
    if upper:

        @pl.when(tok >= tok_count // 2)
        def _():
            mask_copy.start()
            load(upper)
            turn_mask()
            work(upper)


def merged(values, keep, plan, groups, tok_count, always=(), lower=(), upper=(), before=()):
    rows_dev = values.shape[2]
    rounds = rows_dev // (PAGE * tok_count)
    head_group = KVH // groups
    count = len(always) + len(lower) + len(upper)
    return pl.pallas_call(
        functools.partial(
            merge_kernel, plan=plan, always=tuple(always), lower=tuple(lower), upper=tuple(upper),
            groups=groups, tok_count=tok_count, rounds=rounds,
        ),
        in_specs=[pl.BlockSpec(memory_space=pltpu.HBM)] * 2 + [pl.BlockSpec(memory_space=pltpu.VMEM) for _ in before],
        out_specs=[pl.BlockSpec(memory_space=pltpu.VMEM) for _ in plan],
        out_shape=[
            jax.ShapeDtypeStruct((len(entry), rounds, head_group, 2, 2, PAGE, HD), jnp.bfloat16)
            for entry in plan
        ],
        scratch_shapes=[
            pltpu.VMEM((count, rounds, 2, 2, PAGE, values.shape[3]), jnp.bfloat16),
            pltpu.VMEM((1, rows_dev), jnp.int32),
            pltpu.VMEM((rows_dev, HD), jnp.float32),
            pltpu.SemaphoreType.DMA((count, rounds)),
            pltpu.SemaphoreType.DMA(()),
        ],
        input_output_aliases={2 + n: n for n in range(len(before))},
        compiler_params=pltpu.CompilerParams(vmem_limit_bytes=VMEM_GRANT),
    )(*[pltpu.with_memory_space_constraint(array, pltpu.HBM) for array in (keep, values)], *before)


def place_kernel(*rest, plan, rounds, chained):
    pieces = rest[: len(plan)]
    out_ref, sems = rest[len(plan) + chained :]
    layer, tok = lax.axis_index("layer"), lax.axis_index("tok")

    def copies():
        n = 0
        for piece_ref, entry in zip(pieces, plan):
            for slot, offset in enumerate(entry):
                if offset is None:
                    continue
                j, k = offset
                for r in range(rounds):
                    pair = pl.ds((layer ^ j) * 2, 2)
                    rows = pl.ds(pl.multiple_of(((tok ^ k) * rounds + r) * PAGE, PAGE), PAGE)
                    yield pltpu.make_async_copy(
                        piece_ref.at[slot, r], out_ref.at[:, pair, :, rows, :], sems.at[n]
                    )
                    n += 1

    for copy in copies():
        copy.start()
    for copy in copies():
        copy.wait()


def placed(pieces, groups, rows_dev, before=None):
    arrays, plan = [array for array, _ in pieces], [entry for _, entry in pieces]
    rounds, head_group = arrays[0].shape[1], arrays[0].shape[2]
    count = sum(len(entry) for entry in plan) * rounds
    chained = before is not None
    return pl.pallas_call(
        functools.partial(place_kernel, plan=plan, rounds=rounds, chained=int(chained)),
        in_specs=[pl.BlockSpec(memory_space=pltpu.VMEM) for _ in arrays]
        + [pl.BlockSpec(memory_space=pltpu.HBM)] * chained,
        out_specs=pl.BlockSpec(memory_space=pltpu.HBM),
        out_shape=jax.ShapeDtypeStruct((head_group, 2 * groups, 2, rows_dev, HD), jnp.bfloat16),
        scratch_shapes=[pltpu.SemaphoreType.DMA((count,))],
        input_output_aliases={len(arrays): 0} if chained else {},
        compiler_params=pltpu.CompilerParams(vmem_limit_bytes=VMEM_GRANT),
    )(*arrays, *([before] if chained else []))


def offsets_of(groups, tok_count):
    half, quarter = tok_count // 2, tok_count // 4
    small = list(range(quarter))
    middle = list(range(quarter, half))
    early = list(range(half, half + quarter))
    late = list(range(half + quarter, tok_count))
    return list(range(groups - 1, 0, -1)), small, middle, early, late


def one_sequence(values, keep, lengths, groups, tok_count):
    rows_dev = values.shape[2]
    _, small, middle, early, late = offsets_of(groups, tok_count)
    layers = range(groups)

    def over_layer(array, j):
        return lax.ppermute(array, "layer", [(i, i ^ j) for i in range(groups)])

    def over_tok(array, k):
        return lax.ppermute(array, "tok", [(i, i ^ k) for i in range(tok_count)])

    def joined(arrays, n):
        return jnp.concatenate([array[n : n + 1] for array in arrays])

    def without_padding(array, k, source):
        rounds = array.shape[1]
        first = source * rows_dev + (source ^ k) * PAGE
        shape = (1, rounds, 1, 1, 1, PAGE, HD)
        position = first + lax.broadcasted_iota(jnp.int32, shape, 5)
        position += lax.broadcasted_iota(jnp.int32, shape, 1) * (PAGE * tok_count)
        return jnp.where(position < lengths[0], array, jnp.zeros_like(array))

    tok = lax.axis_index("tok")
    first = merged(
        values, keep, [[(j, k) for j in layers] for k in early] + [[(j, k) for k in late] for j in layers],
        groups, tok_count, always=early + late,
    )
    lengths, first = lax.optimization_barrier((lengths, first))
    second = merged(
        values, keep, [[(j, k) for k in middle] for j in layers] + [[(j, k) for j in layers] for k in small],
        groups, tok_count, always=middle + small,
    )
    early_in = [over_tok(array, k) for array, k in zip(first, early)]
    early_in = [without_padding(array, k, tok ^ k) for array, k in zip(early_in, early)]

    def at_home(arrays):
        return [arrays[0]] + [over_layer(arrays[j], j) for j in layers if j]

    late_mine = at_home(first[len(early) :])
    middle_mine = at_home(second[:groups])
    small_in = [over_tok(array, k) if k else array for array, k in zip(second[groups:], small)]
    small_in = [without_padding(array, k, tok ^ k) for array, k in zip(small_in, small)]
    small_mine = [over_layer(joined(small_in, j), j) for j in layers if j]

    def ready(arrays, n, k):
        return without_padding(joined(arrays, n), k, tok)

    late_in = [over_tok(ready(late_mine, n, k), k) for n, k in enumerate(late)]
    middle_in = [over_tok(ready(middle_mine, n, k), k) for n, k in enumerate(middle)]
    early_mine = [over_layer(joined(early_in, j), j) for j in layers if j]
    out = placed(
        [(array[:1], [(0, k)]) for array, k in zip(early_in + small_in, early + small)]
        + [(array, [(j, k) for k in small]) for array, j in zip(small_mine, layers[1:])],
        groups, rows_dev,
    )
    return placed(
        [(array, [(j, k) for j in layers]) for array, k in zip(late_in + middle_in, late + middle)]
        + [(array, [(j, k) for k in early]) for array, j in zip(early_mine, layers[1:])],
        groups, rows_dev, before=out,
    )


def shards(kv_cache, keep_mask, lengths):
    groups = lax.axis_size("layer")
    tok_count = lax.axis_size("tok")
    seq_count = kv_cache.shape[3]
    return jnp.stack(
        [
            one_sequence(kv_cache[0, :, :, s], keep_mask[0, s : s + 1], lengths[s : s + 1], groups, tok_count)
            for s in range(seq_count)
        ]
    )


def solution(mesh):
    in_specs = (P("layer", None, None, None, "tok", None), P("layer", None, "tok"), P())
    out_specs = P(None, "layer", None, None, "tok", None)
    return jax.shard_map(shards, mesh=mesh, in_specs=in_specs, out_specs=out_specs, check_vma=False)
```

```python
import functools

import jax
import jax.numpy as jnp
from jax import lax
from jax.experimental import pallas as pl
from jax.experimental.pallas import tpu as pltpu
from jax.sharding import PartitionSpec as P


KVH = 8
HD = 128
PAGE = 16


epsilon = 1e-06

VMEM_GRANT = 16 * 2**20


def mean_square(x):
    return jnp.mean(x * x, axis=-1, keepdims=True) + epsilon


def merge_kernel(keep_ref, values_ref, *rest, plan, always, lower, upper, groups, tok_count, rounds):
    loaded, mask, columns, squares, sems, mask_sem = rest[-6:]
    outs = rest[-6 - len(plan) : -6]
    layer, tok = lax.axis_index("layer"), lax.axis_index("tok")
    rows_dev = values_ref.shape[2]
    head_group = KVH // groups
    width = head_group * HD
    where = {}
    for o, entry in enumerate(plan):
        for n, piece in enumerate(entry):
            where[piece] = (o, n)
    slots = {k: n for n, k in enumerate(always + lower + upper)}

    def copies(k):
        n = slots[k]
        for r in range(rounds):
            source = pl.ds(pl.multiple_of((r * tok_count + (tok ^ k)) * PAGE, PAGE), PAGE)
            yield pltpu.make_async_copy(values_ref.at[:, :, source, :], loaded.at[n, r], sems.at[n, r])

    mask_copy = pltpu.make_async_copy(keep_ref, mask, mask_sem)

    def load(offsets):
        for k in offsets:
            for copy in copies(k):
                copy.start()

    def turn_mask():
        mask_copy.wait()
        for block in range(0, rows_dev, HD):
            keep = (mask[:, block : block + HD] > 0).astype(jnp.float32)
            columns[block : block + HD, :] = jnp.broadcast_to(keep, (HD, HD)).T

    def work(offsets):
        def parts(k):
            for r in range(rounds):
                for j in range(groups):
                    for c in range(2):
                        for member in range(head_group):
                            yield slots[k], r, j, c, member

        def read(n, r, side, j, c, member):
            lane = pl.multiple_of((layer ^ j) * width + member * HD, HD)
            return loaded[n, r, side, c, :, pl.ds(lane, HD)].astype(jnp.float32)

        def put(at, which, value):
            squares[at + (which,)] = jnp.broadcast_to(value, (PAGE, HD))

        def total(n, r, j, c, member):
            at = (n, r, j, c, member)
            lower = read(n, r, 0, j, c, member) * lax.rsqrt(squares[at + (0,)])
            return lower + read(n, r, 1, j, c, member) * lax.rsqrt(squares[at + (1,)])

        def singles(k):
            pass
            for at in parts(k):
                n, r, j, c, member = at
                for side in range(2):
                    put(at, side, mean_square(read(n, r, side, j, c, member)))

        def sums(k):
            for at in parts(k):
                put(at, 2, mean_square(total(*at)))

        def results(k):
            for at in parts(k):
                n, r, j, c, member = at
                start = pl.multiple_of((r * tok_count + (tok ^ k)) * PAGE, PAGE)
                retained = columns[pl.ds(start, PAGE), :] > 0.0
                direction = total(*at) * lax.rsqrt(squares[at + (2,)])
                o, slot = where[(j, k)]
                for side in range(2):
                    square = squares[at + (side,)]
                    scaled = (square * lax.rsqrt(square)) * direction
                    chosen = jnp.where(retained, read(n, r, side, j, c, member), scaled)
                    outs[o][slot, r, member, side, c] = chosen.astype(jnp.bfloat16)

        for k in offsets:
            for copy in copies(k):
                copy.wait()
        for step in range(len(offsets) + 2):
            if step < len(offsets):
                singles(offsets[step])
            if 0 <= step - 1 < len(offsets):
                sums(offsets[step - 1])
            if 0 <= step - 2:
                results(offsets[step - 2])

    if always:
        mask_copy.start()
        load(always)
        if lower:
            pl.when(tok < tok_count // 2)(lambda: load(lower))
        turn_mask()
        work(always)
        if lower:
            pl.when(tok < tok_count // 2)(lambda: work(lower))
    if upper:

        @pl.when(tok >= tok_count // 2)
        def _():
            mask_copy.start()
            load(upper)
            turn_mask()
            work(upper)


def merged(values, keep, plan, groups, tok_count, always=(), lower=(), upper=(), before=()):
    rows_dev = values.shape[2]
    rounds = rows_dev // (PAGE * tok_count)
    head_group = KVH // groups
    count = len(always) + len(lower) + len(upper)
    return pl.pallas_call(
        functools.partial(
            merge_kernel, plan=plan, always=tuple(always), lower=tuple(lower), upper=tuple(upper),
            groups=groups, tok_count=tok_count, rounds=rounds,
        ),
        in_specs=[pl.BlockSpec(memory_space=pltpu.HBM)] * 2 + [pl.BlockSpec(memory_space=pltpu.VMEM) for _ in before],
        out_specs=[pl.BlockSpec(memory_space=pltpu.VMEM) for _ in plan],
        out_shape=[
            jax.ShapeDtypeStruct((len(entry), rounds, head_group, 2, 2, PAGE, HD), jnp.bfloat16)
            for entry in plan
        ],
        scratch_shapes=[
            pltpu.VMEM((count, rounds, 2, 2, PAGE, values.shape[3]), jnp.bfloat16),
            pltpu.VMEM((1, rows_dev), jnp.int32),
            pltpu.VMEM((rows_dev, HD), jnp.float32),
            pltpu.VMEM((count, rounds, groups, 2, head_group, 3, PAGE, HD), jnp.float32),
            pltpu.SemaphoreType.DMA((count, rounds)),
            pltpu.SemaphoreType.DMA(()),
        ],
        input_output_aliases={2 + n: n for n in range(len(before))},
        compiler_params=pltpu.CompilerParams(vmem_limit_bytes=VMEM_GRANT),
    )(*[pltpu.with_memory_space_constraint(array, pltpu.HBM) for array in (keep, values)], *before)


def place_kernel(*rest, plan, rounds, chained):
    pieces = rest[: len(plan)]
    out_ref, sems = rest[len(plan) + chained :]
    layer, tok = lax.axis_index("layer"), lax.axis_index("tok")

    def copies():
        n = 0
        for piece_ref, entry in zip(pieces, plan):
            for slot, offset in enumerate(entry):
                if offset is None:
                    continue
                j, k = offset
                for r in range(rounds):
                    pair = pl.ds((layer ^ j) * 2, 2)
                    rows = pl.ds(pl.multiple_of(((tok ^ k) * rounds + r) * PAGE, PAGE), PAGE)
                    yield pltpu.make_async_copy(
                        piece_ref.at[slot, r], out_ref.at[:, pair, :, rows, :], sems.at[n]
                    )
                    n += 1

    for copy in copies():
        copy.start()
    for copy in copies():
        copy.wait()


def placed(pieces, groups, rows_dev, before=None):
    arrays, plan = [array for array, _ in pieces], [entry for _, entry in pieces]
    rounds, head_group = arrays[0].shape[1], arrays[0].shape[2]
    count = sum(len(entry) for entry in plan) * rounds
    chained = before is not None
    return pl.pallas_call(
        functools.partial(place_kernel, plan=plan, rounds=rounds, chained=int(chained)),
        in_specs=[pl.BlockSpec(memory_space=pltpu.VMEM) for _ in arrays]
        + [pl.BlockSpec(memory_space=pltpu.HBM)] * chained,
        out_specs=pl.BlockSpec(memory_space=pltpu.HBM),
        out_shape=jax.ShapeDtypeStruct((head_group, 2 * groups, 2, rows_dev, HD), jnp.bfloat16),
        scratch_shapes=[pltpu.SemaphoreType.DMA((count,))],
        input_output_aliases={len(arrays): 0} if chained else {},
        compiler_params=pltpu.CompilerParams(vmem_limit_bytes=VMEM_GRANT),
    )(*arrays, *([before] if chained else []))


def offsets_of(groups, tok_count):
    half, quarter = tok_count // 2, tok_count // 4
    small = list(range(quarter))
    middle = list(range(quarter, half))
    early = list(range(half, half + quarter))
    late = list(range(half + quarter, tok_count))
    return list(range(groups - 1, 0, -1)), small, middle, early, late


def one_sequence(values, keep, lengths, groups, tok_count):
    rows_dev = values.shape[2]
    _, small, middle, early, late = offsets_of(groups, tok_count)
    layers = range(groups)

    def over_layer(array, j):
        return lax.ppermute(array, "layer", [(i, i ^ j) for i in range(groups)])

    def over_tok(array, k):
        return lax.ppermute(array, "tok", [(i, i ^ k) for i in range(tok_count)])

    def joined(arrays, n):
        return jnp.concatenate([array[n : n + 1] for array in arrays])

    def without_padding(array, k, source):
        rounds = array.shape[1]
        first = source * rows_dev + (source ^ k) * PAGE
        shape = (1, rounds, 1, 1, 1, PAGE, HD)
        position = first + lax.broadcasted_iota(jnp.int32, shape, 5)
        position += lax.broadcasted_iota(jnp.int32, shape, 1) * (PAGE * tok_count)
        return jnp.where(position < lengths[0], array, jnp.zeros_like(array))

    tok = lax.axis_index("tok")
    first = merged(
        values, keep, [[(j, k) for j in layers] for k in early] + [[(j, k) for k in late] for j in layers],
        groups, tok_count, always=early + late,
    )
    lengths, first = lax.optimization_barrier((lengths, first))
    second = merged(
        values, keep, [[(j, k) for k in middle] for j in layers] + [[(j, k) for j in layers] for k in small],
        groups, tok_count, always=middle + small,
    )
    early_in = [over_tok(array, k) for array, k in zip(first, early)]
    early_in = [without_padding(array, k, tok ^ k) for array, k in zip(early_in, early)]

    def at_home(arrays):
        return [arrays[0]] + [over_layer(arrays[j], j) for j in layers if j]

    late_mine = at_home(first[len(early) :])
    middle_mine = at_home(second[:groups])
    small_in = [over_tok(array, k) if k else array for array, k in zip(second[groups:], small)]
    small_in = [without_padding(array, k, tok ^ k) for array, k in zip(small_in, small)]
    small_mine = [over_layer(joined(small_in, j), j) for j in layers if j]

    def ready(arrays, n, k):
        return without_padding(joined(arrays, n), k, tok)

    late_in = [over_tok(ready(late_mine, n, k), k) for n, k in enumerate(late)]
    middle_in = [over_tok(ready(middle_mine, n, k), k) for n, k in enumerate(middle)]
    early_mine = [over_layer(joined(early_in, j), j) for j in layers if j]
    out = placed(
        [(array[:1], [(0, k)]) for array, k in zip(early_in + small_in, early + small)]
        + [(array, [(j, k) for k in small]) for array, j in zip(small_mine, layers[1:])],
        groups, rows_dev,
    )
    return placed(
        [(array, [(j, k) for j in layers]) for array, k in zip(late_in + middle_in, late + middle)]
        + [(array, [(j, k) for k in early]) for array, j in zip(early_mine, layers[1:])],
        groups, rows_dev, before=out,
    )


def shards(kv_cache, keep_mask, lengths):
    groups = lax.axis_size("layer")
    tok_count = lax.axis_size("tok")
    seq_count = kv_cache.shape[3]
    return jnp.stack(
        [
            one_sequence(kv_cache[0, :, :, s], keep_mask[0, s : s + 1], lengths[s : s + 1], groups, tok_count)
            for s in range(seq_count)
        ]
    )


def solution(mesh):
    in_specs = (P("layer", None, None, None, "tok", None), P("layer", None, "tok"), P())
    out_specs = P(None, "layer", None, None, "tok", None)
    return jax.shard_map(shards, mesh=mesh, in_specs=in_specs, out_specs=out_specs, check_vma=False)
```

```python
import functools

import jax
import jax.numpy as jnp
from jax import lax
from jax.experimental import pallas as pl
from jax.experimental.pallas import tpu as pltpu
from jax.sharding import PartitionSpec as P


KVH = 8
HD = 128
PAGE = 16


epsilon = 1e-06

VMEM_GRANT = 16 * 2**20


def mean_square(x):
    return jnp.mean(x * x, axis=-1, keepdims=True) + epsilon


def merge_kernel(keep_ref, values_ref, *rest, plan, always, lower, upper, groups, tok_count, rounds):
    loaded, mask, columns, squares, sems, mask_sem = rest[-6:]
    outs = rest[-6 - len(plan) : -6]
    layer, tok = lax.axis_index("layer"), lax.axis_index("tok")
    rows_dev = values_ref.shape[2]
    head_group = KVH // groups
    width = head_group * HD
    where = {}
    for o, entry in enumerate(plan):
        for n, piece in enumerate(entry):
            where[piece] = (o, n)
    slots = {k: n for n, k in enumerate(always + lower + upper)}

    def copies(k):
        n = slots[k]
        for r in range(rounds):
            source = pl.ds(pl.multiple_of((r * tok_count + (tok ^ k)) * PAGE, PAGE), PAGE)
            yield pltpu.make_async_copy(values_ref.at[:, :, source, :], loaded.at[n, r], sems.at[n, r])

    mask_copy = pltpu.make_async_copy(keep_ref, mask, mask_sem)

    def load(offsets):
        for k in offsets:
            for copy in copies(k):
                copy.start()

    def turn_mask():
        mask_copy.wait()
        for block in range(0, rows_dev, HD):
            keep = (mask[:, block : block + HD] > 0).astype(jnp.float32)
            columns[block : block + HD, :] = jnp.broadcast_to(keep, (HD, HD)).T

    def work(offsets):
        def parts(k):
            for r in range(rounds):
                for j in range(groups):
                    for c in range(2):
                        for member in range(head_group):
                            yield slots[k], r, j, c, member

        def read(n, r, side, j, c, member):
            lane = pl.multiple_of((layer ^ j) * width + member * HD, HD)
            return loaded[n, r, side, c, :, pl.ds(lane, HD)].astype(jnp.float32)

        def put(at, which, value):
            squares[at + (which,)] = jnp.broadcast_to(value, (PAGE, HD))

        def total(n, r, j, c, member):
            at = (n, r, j, c, member)
            lower = read(n, r, 0, j, c, member) * lax.rsqrt(squares[at + (0,)])
            return lower + read(n, r, 1, j, c, member) * lax.rsqrt(squares[at + (1,)])

        def singles(k):
            pass
            for at in parts(k):
                n, r, j, c, member = at
                for side in range(2):
                    put(at, side, mean_square(read(n, r, side, j, c, member)))

        def sums(k):
            for at in parts(k):
                put(at, 2, mean_square(total(*at)))

        def results(k):
            for at in parts(k):
                n, r, j, c, member = at
                start = pl.multiple_of((r * tok_count + (tok ^ k)) * PAGE, PAGE)
                retained = columns[pl.ds(start, PAGE), :] > 0.0
                direction = total(*at) * lax.rsqrt(squares[at + (2,)])
                o, slot = where[(j, k)]
                for side in range(2):
                    square = squares[at + (side,)]
                    scaled = (square * lax.rsqrt(square)) * direction
                    chosen = jnp.where(retained, read(n, r, side, j, c, member), scaled)
                    outs[o][slot, r, member, side, c] = chosen.astype(jnp.bfloat16)

        for k in offsets:
            for copy in copies(k):
                copy.wait()
        for step in range(len(offsets) + 2):
            if step < len(offsets):
                singles(offsets[step])
            if 0 <= step - 1 < len(offsets):
                sums(offsets[step - 1])
            if 0 <= step - 2:
                results(offsets[step - 2])

    if always:
        mask_copy.start()
        load(always)
        if lower:
            pl.when(tok < tok_count // 2)(lambda: load(lower))
        turn_mask()
        work(always)
        if lower:
            pl.when(tok < tok_count // 2)(lambda: work(lower))
    if upper:

        @pl.when(tok >= tok_count // 2)
        def _():
            mask_copy.start()
            load(upper)
            turn_mask()
            work(upper)


def merged(values, keep, plan, groups, tok_count, always=(), lower=(), upper=(), before=()):
    rows_dev = values.shape[2]
    rounds = rows_dev // (PAGE * tok_count)
    head_group = KVH // groups
    count = len(always) + len(lower) + len(upper)
    return pl.pallas_call(
        functools.partial(
            merge_kernel, plan=plan, always=tuple(always), lower=tuple(lower), upper=tuple(upper),
            groups=groups, tok_count=tok_count, rounds=rounds,
        ),
        in_specs=[pl.BlockSpec(memory_space=pltpu.HBM)] * 2 + [pl.BlockSpec(memory_space=pltpu.VMEM) for _ in before],
        out_specs=[pl.BlockSpec(memory_space=pltpu.VMEM) for _ in plan],
        out_shape=[
            jax.ShapeDtypeStruct((len(entry), rounds, head_group, 2, 2, PAGE, HD), jnp.bfloat16)
            for entry in plan
        ],
        scratch_shapes=[
            pltpu.VMEM((count, rounds, 2, 2, PAGE, values.shape[3]), jnp.bfloat16),
            pltpu.VMEM((1, rows_dev), jnp.int32),
            pltpu.VMEM((rows_dev, HD), jnp.float32),
            pltpu.VMEM((count, rounds, groups, 2, head_group, 3, PAGE, HD), jnp.float32),
            pltpu.SemaphoreType.DMA((count, rounds)),
            pltpu.SemaphoreType.DMA(()),
        ],
        input_output_aliases={2 + n: n for n in range(len(before))},
        compiler_params=pltpu.CompilerParams(vmem_limit_bytes=VMEM_GRANT),
    )(*[pltpu.with_memory_space_constraint(array, pltpu.HBM) for array in (keep, values)], *before)


def place_kernel(*rest, plan, rounds, chained):
    pieces = rest[: len(plan)]
    out_ref, sems = rest[len(plan) + chained :]
    layer, tok = lax.axis_index("layer"), lax.axis_index("tok")

    def copies():
        n = 0
        for piece_ref, entry in zip(pieces, plan):
            for slot, offset in enumerate(entry):
                if offset is None:
                    continue
                j, k = offset
                for r in range(rounds):
                    pair = pl.ds((layer ^ j) * 2, 2)
                    rows = pl.ds(pl.multiple_of(((tok ^ k) * rounds + r) * PAGE, PAGE), PAGE)
                    yield pltpu.make_async_copy(
                        piece_ref.at[slot, r], out_ref.at[:, pair, :, rows, :], sems.at[n]
                    )
                    n += 1

    for copy in copies():
        copy.start()
    for copy in copies():
        copy.wait()


def placed(pieces, groups, rows_dev, before=None):
    arrays, plan = [array for array, _ in pieces], [entry for _, entry in pieces]
    rounds, head_group = arrays[0].shape[1], arrays[0].shape[2]
    count = sum(len(entry) for entry in plan) * rounds
    chained = before is not None
    return pl.pallas_call(
        functools.partial(place_kernel, plan=plan, rounds=rounds, chained=int(chained)),
        in_specs=[pl.BlockSpec(memory_space=pltpu.VMEM) for _ in arrays]
        + [pl.BlockSpec(memory_space=pltpu.HBM)] * chained,
        out_specs=pl.BlockSpec(memory_space=pltpu.HBM),
        out_shape=jax.ShapeDtypeStruct((head_group, 2 * groups, 2, rows_dev, HD), jnp.bfloat16),
        scratch_shapes=[pltpu.SemaphoreType.DMA((count,))],
        input_output_aliases={len(arrays): 0} if chained else {},
        compiler_params=pltpu.CompilerParams(vmem_limit_bytes=VMEM_GRANT),
    )(*arrays, *([before] if chained else []))


def offsets_of(groups, tok_count):
    half, quarter = tok_count // 2, tok_count // 4
    small = list(range(quarter))
    middle = list(range(quarter, half))
    early = list(range(half, half + quarter))
    late = list(range(half + quarter, tok_count))
    return list(range(groups - 1, 0, -1)), small, middle, early, late


def one_sequence(values, keep, lengths, groups, tok_count):
    rows_dev = values.shape[2]
    _, small, middle, early, late = offsets_of(groups, tok_count)
    layers = range(groups)

    def over_layer(array, j):
        return lax.ppermute(array, "layer", [(i, i ^ j) for i in range(groups)])

    def over_tok(array, k):
        return lax.ppermute(array, "tok", [(i, i ^ k) for i in range(tok_count)])

    def joined(arrays, n):
        return jnp.concatenate([array[n : n + 1] for array in arrays])

    def without_padding(array, k, source):
        rounds = array.shape[1]
        first = source * rows_dev + (source ^ k) * PAGE
        shape = (1, rounds, 1, 1, 1, PAGE, HD)
        position = first + lax.broadcasted_iota(jnp.int32, shape, 5)
        position += lax.broadcasted_iota(jnp.int32, shape, 1) * (PAGE * tok_count)
        return jnp.where(position < lengths[0], array, jnp.zeros_like(array))

    tok = lax.axis_index("tok")
    first = merged(
        values, keep, [[(j, k) for j in layers] for k in early] + [[(j, k) for k in late] for j in layers],
        groups, tok_count, always=early + late,
    )
    lengths, first = lax.optimization_barrier((lengths, first))
    second = merged(
        values, keep, [[(j, k) for k in middle] for j in layers] + [[(j, k) for j in layers] for k in small],
        groups, tok_count, always=middle + small,
    )
    early_in = [over_tok(array, k) for array, k in zip(first, early)]
    early_in = [without_padding(array, k, tok ^ k) for array, k in zip(early_in, early)]

    def at_home(arrays):
        return [arrays[0]] + [over_layer(arrays[j], j) for j in layers if j]

    late_mine = at_home(first[len(early) :])
    middle_mine = at_home(second[:groups])
    small_in = [over_tok(array, k) if k else array for array, k in zip(second[groups:], small)]
    small_in = [without_padding(array, k, tok ^ k) for array, k in zip(small_in, small)]
    small_mine = [over_layer(joined(small_in, j), j) for j in layers if j]

    late_in = [over_tok(joined(late_mine, n), k) for n, k in enumerate(late)]
    late_in = [without_padding(array, k, tok ^ k) for array, k in zip(late_in, late)]
    middle_out = [without_padding(joined(middle_mine, n), k, tok) for n, k in enumerate(middle)]
    middle_in = [over_tok(array, k) for array, k in zip(middle_out, middle)]
    early_mine = [over_layer(joined(early_in, j), j) for j in layers if j]
    out = placed(
        [(array[:1], [(0, k)]) for array, k in zip(early_in + small_in, early + small)]
        + [(array, [(j, k) for k in small]) for array, j in zip(small_mine, layers[1:])],
        groups, rows_dev,
    )
    return placed(
        [(array, [(j, k) for j in layers]) for array, k in zip(late_in + middle_in, late + middle)]
        + [(array, [(j, k) for k in early]) for array, j in zip(early_mine, layers[1:])],
        groups, rows_dev, before=out,
    )


def shards(kv_cache, keep_mask, lengths):
    groups = lax.axis_size("layer")
    tok_count = lax.axis_size("tok")
    seq_count = kv_cache.shape[3]
    return jnp.stack(
        [
            one_sequence(kv_cache[0, :, :, s], keep_mask[0, s : s + 1], lengths[s : s + 1], groups, tok_count)
            for s in range(seq_count)
        ]
    )


def solution(mesh):
    in_specs = (P("layer", None, None, None, "tok", None), P("layer", None, "tok"), P())
    out_specs = P(None, "layer", None, None, "tok", None)
    return jax.shard_map(shards, mesh=mesh, in_specs=in_specs, out_specs=out_specs, check_vma=False)
```
